32 devices in a mesh: win: 2 (over core), grp: 16 (over z, y, x).
Axes of the slice: x: 2, y: 2, z: 4, core: 2. Of those that a mesh axis runs over, the one named last changes fastest.
Arguments:
- atom_table: float32 [4, 6, 24576], P('win', None, 'grp'), as said below
- row_blocks: int32 [4, 1024], P('win', 'grp'), may hold values from 0 to 191, as said below
- col_blocks: int32 [4, 1024], P('win', 'grp'), may hold values from 0 to 191, as said below
- lambdas: float32 [4], replicated, may hold values from 0 to 1, as said below
- inverse_temp: float32 [1], replicated, may hold values from 20 to 80
- parity: int32 [1], replicated, may hold values from 0 to 1073741823
- thresholds: int32 [4], replicated, may hold values from 0 to 1073741823
Outputs:
- energies: float32 [4, 3], P('win')
- margins: float32 [4], P('win')
- profile: float32 [4], P('win')
The draws below stay inside these ranges and needn't reach their ends.
Inputs may be any that keep to these rules, and one draw needn't show every extreme that they name: `row_blocks`: the first block of each pair listed on index g of grp lies in that index's share of atoms: blocks g * 12 to (g + 1) * 12 - 1. `col_blocks`: the list of one index of grp names blocks of any one index of grp (itself included) at most 5 times; in each window some index of grp has exactly 5 of its blocks named in every list of that window. `lambdas`: strictly increasing. `atom_table`: field 4 lies in 0.7 to 1.4 and field 5 in 0.6 to 1.4.
All inputs are finite; a program needn't handle non-finite values.
Results may differ from the reference program's by a relative error of at most 0.0003.
Values sent between devices are 32-bit elements; how exact they have to be, the bound alone decides.
A program may use at most 64 MiB of HBM per device.

```python
import math
import jax
import jax.numpy as jnp
from jax import lax

TILE = 128
BLK_DEV = 12
PB_DEV = 64
WINDOWS = 4
BLOCKS = 192
ATOMS = 24576
PAIRS = 1024
SLOTS = 5


def draw_atom_table(key, part):
    keys = jax.random.split(key, 12)
    regions = BLOCKS // BLK_DEV
    centres = jax.random.uniform(keys[0], (WINDOWS, 3, BLOCKS, 1), minval=-1.5, maxval=1.5)
    radius = jnp.exp(jax.random.uniform(keys[1], (WINDOWS, 1, BLOCKS, 1), minval=jnp.log(0.25), maxval=jnp.log(0.9)))
    offsets = jax.random.normal(keys[2], (WINDOWS, 3, BLOCKS, TILE))
    region_charge = 0.3 + 0.6 * jax.random.normal(keys[3], (WINDOWS, regions))
    block_charge = 0.3 * jax.random.normal(keys[4], (WINDOWS, BLOCKS))
    atom_charge = 0.3 * jax.random.normal(keys[5], (WINDOWS, BLOCKS, TILE))
    coords = (centres + radius * offsets).reshape(WINDOWS, 3, ATOMS)
    charge_block = jnp.repeat(region_charge, BLK_DEV, axis=1) + block_charge
    charge = (charge_block[:, :, None] + atom_charge).reshape(WINDOWS, 1, ATOMS)
    depth_block = jnp.exp(jax.random.uniform(keys[6], (WINDOWS, BLOCKS, 1), minval=jnp.log(0.75), maxval=jnp.log(1.3)))
    depth_atom = jnp.exp(jax.random.uniform(keys[7], (WINDOWS, BLOCKS, TILE), minval=jnp.log(0.935), maxval=jnp.log(1.07)))
    depth_root = (depth_block * depth_atom).reshape(WINDOWS, 1, ATOMS)
    size_block = jax.random.uniform(keys[8], (WINDOWS, BLOCKS, 1), minval=0.65, maxval=1.35)
    size_atom = jax.random.uniform(keys[9], (WINDOWS, BLOCKS, TILE), minval=-0.05, maxval=0.05)
    size_sq = (size_block + size_atom).reshape(WINDOWS, 1, ATOMS)
    return jnp.concatenate([coords, charge, depth_root, size_sq], axis=1).astype(jnp.float32)


def draw_row_blocks(key, part):
    offset = jnp.arange(PAIRS, dtype=jnp.int32) // PB_DEV * BLK_DEV
    picks = jax.random.randint(key, (WINDOWS, PAIRS), 0, BLK_DEV, dtype=jnp.int32)
    return picks + offset[None, :]


def draw_col_blocks(key, part):
    groups = PAIRS // PB_DEV
    pool = jnp.arange(groups * SLOTS, dtype=jnp.int32) // SLOTS
    keys = jax.random.split(jax.random.fold_in(key, 7), 2)
    heavy = jax.random.randint(keys[0], (WINDOWS,), 0, groups, dtype=jnp.int32)
    list_keys = jax.random.split(keys[1], WINDOWS * groups)

    def one_list(list_key, heavy_owner):
        first_key, second_key, third_key = jax.random.split(list_key, 3)
        order = jax.random.permutation(first_key, groups * SLOTS)
        owners = pool[order]
        placed = jnp.argsort((owners != heavy_owner).astype(jnp.int32), stable=True)
        chosen = owners[placed][:PB_DEV]
        chosen = jax.random.permutation(second_key, chosen)
        within = jax.random.randint(third_key, (PB_DEV,), 0, BLK_DEV, dtype=jnp.int32)
        return (chosen * BLK_DEV + within).astype(jnp.int32)
    heavy_rows = jnp.repeat(heavy, groups)
    lists = jax.vmap(one_list)(list_keys, heavy_rows)
    return lists.reshape(WINDOWS, PAIRS).astype(jnp.int32)


def draw_lambdas(key, part):
    keys = jax.random.split(jax.random.fold_in(key, 11), 3)
    increments = jax.random.uniform(keys[0], (WINDOWS,), minval=0.5, maxval=1.5)
    start = jax.random.uniform(keys[1], (), minval=0.0, maxval=0.25)
    finish = jax.random.uniform(keys[2], (), minval=0.75, maxval=1.0)
    running = jnp.cumsum(increments)
    unit = (running - running[0]) / (running[-1] - running[0])
    return (start + (finish - start) * unit).astype(jnp.float32)


def plant(drawn, key, least, largest):
    extent = drawn.shape
    place = [jax.random.randint(jax.random.fold_in(key, axis), (), 0, extent[axis]) for axis in range(len(extent))]
    drawn = drawn.at[tuple(place)].set(least)
    longest = extent.index(max(extent))
    place[longest] = (place[longest] + 1) % extent[longest]
    return drawn.at[tuple(place)].set(largest)


def setup_inputs(seed: int = 0) -> dict:
    seeds = jax.random.split(jax.random.key(seed), 8)
    return {
        "atom_table": draw_atom_table(jax.random.fold_in(seeds[7], 71), 0),
        "row_blocks": draw_row_blocks(jax.random.fold_in(seeds[7], 71), 0),
        "col_blocks": draw_col_blocks(jax.random.fold_in(seeds[7], 71), 0),
        "lambdas": draw_lambdas(jax.random.fold_in(seeds[7], 71), 0),
        "inverse_temp": jnp.clip(jnp.exp(jax.random.uniform(seeds[4], (1,), jnp.float32, math.log(20.0), math.log(80.0))), 20.0, 80.0),
        "parity": jax.random.randint(seeds[5], (1,), 0, 1073741824).astype(jnp.int32),
        "thresholds": plant(jax.random.randint(seeds[6], (WINDOWS,), 0, 1073741824), jax.random.fold_in(seeds[6], 1), 0, 1073741823).astype(jnp.int32),
    }


tiles_per_step = 16

def pair_energy(row_data, col_data, same_block, lambda_set):
    delta_x = row_data[0][:, :, None] - col_data[0][:, None, :]
    delta_y = row_data[1][:, :, None] - col_data[1][:, None, :]
    delta_z = row_data[2][:, :, None] - col_data[2][:, None, :]
    distance = delta_x * delta_x + delta_y * delta_y + delta_z * delta_z
    charge_pair = row_data[3][:, :, None] * col_data[3][:, None, :]
    well_depth = 4.0 * row_data[4][:, :, None] * col_data[4][:, None, :]
    size_pair = row_data[5][:, :, None] * col_data[5][:, None, :]
    scaled = distance / size_pair
    scaled_cube = scaled * scaled * scaled
    width_tile = distance.shape[-1]
    diagonal = (lax.broadcasted_iota(jnp.int32, (width_tile, width_tile), 0) == lax.broadcasted_iota(jnp.int32, (width_tile, width_tile), 1)).astype(jnp.float32)
    keep_mask = 1.0 - same_block[:, None, None] * diagonal[None]
    totals = []
    for number in range(3):
        lam_now = lambda_set[number]
        softened = 1.0 - 0.5 * lam_now + scaled_cube
        inverse = 1.0 / softened
        dispersion = well_depth * (inverse * inverse - inverse)
        coulomb = charge_pair * lax.rsqrt(distance + 2.0 - lam_now)
        totals.append(lam_now * jnp.sum(keep_mask * (dispersion + coulomb)))
    return jnp.stack(totals)

def window_sums(table, row_ids, col_ids, lambda_set):
    blocks = table.reshape(table.shape[0], -1, TILE)
    row_all = jnp.take(blocks, row_ids, axis=1)
    col_all = jnp.take(blocks, col_ids, axis=1)
    same_all = (row_ids == col_ids).astype(jnp.float32)
    count = row_ids.shape[0] // tiles_per_step

    def advance(number, total):
        start = number * tiles_per_step
        row_part = lax.dynamic_slice_in_dim(row_all, start, tiles_per_step, 1)
        col_part = lax.dynamic_slice_in_dim(col_all, start, tiles_per_step, 1)
        same_part = lax.dynamic_slice_in_dim(same_all, start, tiles_per_step, 0)
        return total + pair_energy(row_part, col_part, same_part, lambda_set)
    return lax.fori_loop(0, count, advance, jnp.zeros((3,), jnp.float32))

def reference(atom_table, row_blocks, col_blocks, lambdas, inverse_temp, parity, thresholds):
    windows = lambdas.shape[0]
    window = jnp.arange(windows, dtype=jnp.int32)
    below = jnp.clip(window - 1, 0, windows - 1)
    above = jnp.clip(window + 1, 0, windows - 1)
    lambda_sets = jnp.stack([lambdas[below], lambdas, lambdas[above]], axis=1)
    sums = lax.map(lambda pack: window_sums(pack[0], pack[1], pack[2], pack[3]), (atom_table, row_blocks, col_blocks, lambda_sets))
    energies = sums / (row_blocks.shape[1] * TILE * TILE)
    d_plus = energies[:, 2] - energies[:, 1]
    d_minus = energies[:, 0] - energies[:, 1]
    profile = jnp.concatenate([jnp.zeros((1,), jnp.float32), jnp.cumsum(d_plus)[:-1]])
    lower_win = jnp.where(jnp.remainder(window - parity[0], 2) == 0, window, window - 1)
    upper_win = lower_win + 1
    has_partner = (lower_win >= 0) & (upper_win < windows)
    lower_safe = jnp.clip(lower_win, 0, windows - 1)
    upper_safe = jnp.clip(upper_win, 0, windows - 1)
    change = d_plus[lower_safe] + d_minus[upper_safe]
    offset_draw = jnp.remainder(thresholds[lower_safe] + parity[0], 1073741824).astype(jnp.int32) + 1
    draw_share = offset_draw.astype(jnp.float32) / 1073741824.0
    margins = jnp.where(has_partner, -jnp.log(draw_share) - inverse_temp[0] * change, 0.0)
    return (energies, margins, profile)
```

```python
import functools

import jax
import jax.numpy as jnp
from jax import lax
from jax.experimental import pallas as pl
from jax.experimental.pallas import tpu as pltpu
from jax.sharding import PartitionSpec as P

TILE = 128
ROWS = 8
FIELDS = 6
PIECES = TILE // ROWS
MESH = pl.DeviceIdType.MESH


def grid_of(mesh):
    groups = mesh.shape["grp"]
    try:
        line = mesh.devices[0]
        coords = [tuple(d.coords) for d in line]
        dims = [len({c[a] for c in coords}) for a in (2, 1, 0)]
        base = [min(c[a] for c in coords) for a in (2, 1, 0)]
        want = [
            (base[2] + x, base[1] + y, base[0] + z)
            for z in range(dims[0])
            for y in range(dims[1])
            for x in range(dims[2])
        ]
        if [c[:3] for c in coords] == want:
            return tuple(dims)
    except Exception:
        pass
    return (groups, 1, 1)


def messages_of(dims):
    z, y, x = dims
    first = (z - 1) + (x - 1) + (y - 1)
    second = (z - 1) * (x + y - 2)
    third = z * (x - 1) * (y - 1)
    return first + second + third


def kernel(
    cfg,
    table,
    row_ids,
    col_ids,
    lambdas,
    inverse_temp,
    parity,
    thresholds,
    out_energy,
    out_margin,
    out_profile,
    *scratch,
):
    run, wins, groups, own, listed, dims = cfg
    bufs = scratch[:run]
    rowbs = scratch[run : 2 * run]
    red, send_sem, recv_sem, red_send, red_recv = scratch[2 * run :]
    dim_z, dim_y, dim_x = dims
    devices = wins * groups
    windows = wins * run
    win = lax.axis_index("win")
    grp = lax.axis_index("grp")
    me = win * groups + grp
    my_z = grp // (dim_y * dim_x)
    my_y = (grp // dim_x) % dim_y
    my_x = grp % dim_x
    two_ends = wins == 2 and run == 2

    def window_of(slot):
        if two_ends:
            return jnp.where(win == 0, slot, 1 - slot)
        return slot

    def at(dz, dy, dx):
        return (
            ((my_z + dz) % dim_z) * dim_y + (my_y + dy) % dim_y
        ) * dim_x + (my_x + dx) % dim_x

    barrier = pltpu.get_barrier_semaphore()

    def greet(step, carry):
        other = (me + step) % devices
        pl.semaphore_signal(
            barrier, inc=1, device_id=(other // groups, other % groups), device_id_type=MESH
        )
        return carry

    lax.fori_loop(1, devices, greet, 0)

    def spread(slot):
        local = window_of(slot)

        def one(block, carry):
            start = pl.multiple_of(block * TILE, TILE)
            tile = table[local, :, pl.ds(start, TILE)]
            packed = jnp.concatenate(
                [tile[0:4], 4.0 * tile[4:5], 1.0 / tile[5:6], tile[0:2]], axis=0
            )
            turned = jnp.transpose(packed)
            for field in range(FIELDS):
                wide = jnp.broadcast_to(turned[:, field : field + 1], (TILE, TILE))
                for piece in range(PIECES):
                    rowbs[slot][(block * FIELDS + field) * PIECES + piece] = wide[
                        piece * ROWS : (piece + 1) * ROWS
                    ]
            bufs[slot][grp * own + block] = tile
            return carry

        lax.fori_loop(0, own, one, 0)

    spread(0)

    shares = []
    lowers = []
    for wl in range(run):
        window = win * run + wl
        odd = (window + parity[0]) & 1
        lower = window - odd
        threshold = thresholds[0]
        for v in range(1, windows):
            threshold = jnp.where(lower == v, thresholds[v], threshold)
        drawn = ((threshold + parity[0]) & 1073741823) + 1
        share = jnp.full((ROWS, TILE), drawn, jnp.int32).astype(jnp.float32) * (1.0 / 1073741824.0)
        shares.append(-jnp.log(share))
        lowers.append(lower)

    pl.semaphore_wait(barrier, devices - 1)

    counts = [0] * run

    def share_of(slot, owner):
        return bufs[slot].at[pl.ds(owner * own, own)]

    def descriptor(slot, owner, target, number):
        return pltpu.make_async_remote_copy(
            src_ref=share_of(slot, owner),
            dst_ref=share_of(slot, owner),
            send_sem=send_sem.at[slot, number],
            recv_sem=recv_sem.at[slot, owner],
            device_id={"grp": target},
            device_id_type=MESH,
        )

    sent = []

    def send(slot, owner, target):
        copy = descriptor(slot, owner, target, counts[slot])
        counts[slot] += 1
        copy.start()
        sent.append(copy)

    def arrived(slot, owner):
        descriptor(slot, owner, owner, 0).wait_recv()

    def to_x(slot, owner):
        for dx in range(1, dim_x):
            send(slot, owner, at(0, 0, dx))

    def to_y(slot, owner):
        for dy in range(1, dim_y):
            send(slot, owner, at(0, dy, 0))

    def open_sends(slot):
        for dz in range(1, dim_z):
            send(slot, grp, at(dz, 0, 0))
        to_x(slot, grp)
        to_y(slot, grp)

    def pass_plane(slot, dz):
        for dx in range(1, dim_x):
            owner = at(dz, 0, dx)
            arrived(slot, owner)
            if dz % 2 == 0:
                to_y(slot, owner)
        for dy in range(1, dim_y):
            owner = at(dz, dy, 0)
            arrived(slot, owner)
            if dz % 2 == 1:
                to_x(slot, owner)

    def pass_column(slot):
        for dz in range(1, dim_z):
            owner = at(dz, 0, 0)
            arrived(slot, owner)
            to_x(slot, owner)
            to_y(slot, owner)

    def pass_planes(slot):
        for dz in range(dim_z):
            pass_plane(slot, dz)

    def last_arrivals(slot):
        for dz in range(dim_z):
            for dy in range(1, dim_y):
                for dx in range(1, dim_x):
                    arrived(slot, at(dz, dy, dx))

    def lambda_list(slot):
        window = win * run + window_of(slot)
        if two_ends and slot == 0:
            low = jnp.where(window == 0, 0, window - 1)
            return [lambdas[low], lambdas[low + 1]]
        return [
            lambdas[jnp.maximum(window - 1, 0)],
            lambdas[window],
            lambdas[jnp.minimum(window + 1, windows - 1)],
        ]

    def start_state(slot):
        zero = jnp.zeros((ROWS, TILE), jnp.float32)
        row = jnp.zeros((1, TILE), jnp.float32)
        return tuple(zero for _ in lambda_list(slot)) + (row, row)

    def tiles(slot, first, last, state):
        local = window_of(slot)
        lams = lambda_list(slot)
        cores = [1.0 - 0.5 * lam for lam in lams]
        softs = [2.0 - lam for lam in lams]
        base = grp * own

        def one(pair, state):
            row_id = row_ids[local, pair]
            col_id = col_ids[local, pair]
            col = bufs[slot][col_id]
            mine = jnp.clip(row_id - base, 0, own - 1) * (FIELDS * PIECES)
            fields = [jnp.broadcast_to(col[f : f + 1], (ROWS, TILE)) for f in range(3)]
            charge_col = col[3:4]
            depth_col = col[4:5]
            size_col = jnp.broadcast_to(1.0 / col[5:6], (ROWS, TILE))
            sum_disp = [None] * len(lams)
            sum_coul = [None] * len(lams)
            for piece in range(TILE // ROWS):
                dx = rowbs[slot][mine + piece] - fields[0]
                dy = rowbs[slot][mine + 1 * PIECES + piece] - fields[1]
                dz = rowbs[slot][mine + 2 * PIECES + piece] - fields[2]
                charge = rowbs[slot][mine + 3 * PIECES + piece]
                depth = rowbs[slot][mine + 4 * PIECES + piece]
                r2 = dx * dx + dy * dy + dz * dz
                scaled = r2 * (rowbs[slot][mine + 5 * PIECES + piece] * size_col)
                cube = scaled * scaled * scaled
                for k in range(len(lams)):
                    root = lax.rsqrt(cube + cores[k])
                    inverse = root * root
                    disp = (depth * inverse) * (inverse - 1.0)
                    coul = charge * lax.rsqrt(r2 + softs[k])
                    if piece == 0:
                        sum_disp[k], sum_coul[k] = disp, coul
                    else:
                        sum_disp[k] = sum_disp[k] + disp
                        sum_coul[k] = sum_coul[k] + coul
            totals = [
                state[k] + (sum_disp[k] * depth_col + sum_coul[k] * charge_col)
                for k in range(len(lams))
            ]
            same = jnp.where(row_id == col_id, 1.0, 0.0)
            return tuple(totals) + (
                state[-2] + same * (depth_col * depth_col),
                state[-1] + same * (charge_col * charge_col),
            )

        return lax.fori_loop(first, last, one, state)

    def close(slot, state):
        out = []
        for k, lam in enumerate(lambda_list(slot)):
            core = jnp.full((1, TILE), 1.0 - 0.5 * lam, jnp.float32)
            soft = jnp.full((1, TILE), 2.0 - lam, jnp.float32)
            inverse = 1.0 / core
            own_pairs = state[-2] * (4.0 * inverse * (inverse - 1.0)) + state[-1] * lax.rsqrt(soft)
            line = jnp.sum(state[k], axis=0, keepdims=True) - own_pairs
            out.append(jnp.sum(line, axis=1, keepdims=True) * lam)
        if two_ends and slot == 0:
            out = [out[0], jnp.where(win == 0, out[0], out[1]), out[1]]
        return out

    open_sends(0)
    for slot in range(1, run):
        spread(slot)
        open_sends(slot)
    pass_column(0)
    if run > 1:
        pass_column(1)
    pass_planes(0)
    last_arrivals(0)
    partial = []
    for slot in range(run):
        state = start_state(slot)
        if slot + 1 < run:
            half = (3 * listed) // 8
            state = tiles(slot, 0, half, state)
            if slot > 0:
                pass_column(slot + 1)
            pass_planes(slot + 1)
            state = tiles(slot, half, listed, state)
            last_arrivals(slot + 1)
        else:
            state = tiles(slot, 0, listed, state)
        partial.append(close(slot, state))

    lane = lax.broadcasted_iota(jnp.int32, (1, TILE), 1)
    line = jnp.zeros((1, TILE), jnp.float32)
    for slot in range(run):
        place = window_of(slot) * 3
        for k in range(3):
            line = jnp.where(lane == place + k, partial[slot][k], line)
    red[me] = line

    def share_out(step, carry):
        other = (me + step) % devices
        pltpu.make_async_remote_copy(
            src_ref=red.at[me],
            dst_ref=red.at[me],
            send_sem=red_send.at[step],
            recv_sem=red_recv.at[me],
            device_id=(other // groups, other % groups),
            device_id_type=MESH,
        ).start()
        return carry

    lax.fori_loop(1, devices, share_out, 0)
    for copy in sent:
        copy.wait_send()

    def collect(step, carry):
        other = (me + step) % devices
        copy = pltpu.make_async_remote_copy(
            src_ref=red.at[other],
            dst_ref=red.at[other],
            send_sem=red_send.at[step],
            recv_sem=red_recv.at[other],
            device_id=(other // groups, other % groups),
            device_id_type=MESH,
        )
        copy.wait_recv()
        copy.wait_send()
        return carry

    lax.fori_loop(1, devices, collect, 0)
    scale = 1.0 / (listed * groups * TILE * TILE)
    energy = []
    for part in range(wins):
        total = jnp.sum(red[part * groups : (part + 1) * groups], axis=0) * scale
        for wl in range(run):
            energy.append(
                [jnp.sum(jnp.where(lane == wl * 3 + k, total, 0.0)) for k in range(3)]
            )
    ups = [e[2] - e[1] for e in energy]
    downs = [e[0] - e[1] for e in energy]
    for wl in range(run):
        window = win * run + wl
        for k in range(3):
            value = energy[wl][k]
            for part in range(1, wins):
                value = jnp.where(win == part, energy[part * run + wl][k], value)
            out_energy[wl, k] = value
        profile = jnp.float32(0.0)
        change = jnp.float32(0.0)
        for v in range(windows):
            profile = profile + jnp.where(v < window, ups[v], 0.0)
            change = change + jnp.where(lowers[wl] == v, ups[v], 0.0)
            change = change + jnp.where(lowers[wl] + 1 == v, downs[v], 0.0)
        out_profile[wl] = profile
        partner = jnp.logical_and(lowers[wl] >= 0, lowers[wl] + 1 < windows)
        margin = jnp.max(shares[wl]) - inverse_temp[0] * change
        out_margin[wl] = jnp.where(partner, margin, 0.0)


def per_device(dims, atom_table, row_blocks, col_blocks, lambdas, inverse_temp, parity, thresholds):
    run, fields, atoms = atom_table.shape
    wins = lax.axis_size("win")
    groups = lax.axis_size("grp")
    own = atoms // TILE
    listed = row_blocks.shape[1]
    cfg = (run, wins, groups, own, listed, dims)
    smem = pl.BlockSpec(memory_space=pltpu.SMEM)
    vmem = pl.BlockSpec(memory_space=pltpu.VMEM)
    devices = wins * groups
    scratch = [pltpu.VMEM((groups * own, fields, TILE), jnp.float32) for _ in range(run)]
    scratch += [pltpu.VMEM((own * FIELDS * PIECES, ROWS, TILE), jnp.float32) for _ in range(run)]
    scratch += [
        pltpu.VMEM((devices, 1, TILE), jnp.float32),
        pltpu.SemaphoreType.DMA((run, max(1, messages_of(dims)))),
        pltpu.SemaphoreType.DMA((run, groups)),
        pltpu.SemaphoreType.DMA((devices,)),
        pltpu.SemaphoreType.DMA((devices,)),
    ]
    return pl.pallas_call(
        functools.partial(kernel, cfg),
        out_shape=(
            jax.ShapeDtypeStruct((run, 3), jnp.float32),
            jax.ShapeDtypeStruct((run,), jnp.float32),
            jax.ShapeDtypeStruct((run,), jnp.float32),
        ),
        in_specs=[vmem, smem, smem, smem, smem, smem, smem],
        out_specs=(smem, smem, smem),
        scratch_shapes=scratch,
        compiler_params=pltpu.CompilerParams(
            collective_id=0, has_side_effects=True, vmem_limit_bytes=48 * 1024 * 1024
        ),
    )(atom_table, row_blocks, col_blocks, lambdas, inverse_temp, parity, thresholds)


def solution(mesh):
    return jax.shard_map(
        functools.partial(per_device, grid_of(mesh)),
        mesh=mesh,
        in_specs=(P("win", None, "grp"), P("win", "grp"), P("win", "grp"), P(), P(), P(), P()),
        out_specs=(P("win", None), P("win"), P("win")),
        check_vma=False,
    )
```

```python
import functools

import jax
import jax.numpy as jnp
from jax import lax
from jax.experimental import pallas as pl
from jax.experimental.pallas import tpu as pltpu
from jax.sharding import PartitionSpec as P

TILE = 128
ROWS = 8
FIELDS = 6
PIECES = TILE // ROWS
MESH = pl.DeviceIdType.MESH


def grid_of(mesh):
    groups = mesh.shape["grp"]
    try:
        line = mesh.devices[0]
        coords = [tuple(d.coords) for d in line]
        dims = [len({c[a] for c in coords}) for a in (2, 1, 0)]
        base = [min(c[a] for c in coords) for a in (2, 1, 0)]
        want = [
            (base[2] + x, base[1] + y, base[0] + z)
            for z in range(dims[0])
            for y in range(dims[1])
            for x in range(dims[2])
        ]
        if [c[:3] for c in coords] == want:
            return tuple(dims)
    except Exception:
        pass
    return (groups, 1, 1)


def messages_of(dims):
    z, y, x = dims
    first = (z - 1) + (x - 1) + (y - 1)
    second = (z - 1) * (x + y - 2)
    third = z * (x - 1) * (y - 1)
    return first + second + third


def kernel(
    cfg,
    table,
    row_ids,
    col_ids,
    lambdas,
    inverse_temp,
    parity,
    thresholds,
    out_energy,
    out_margin,
    out_profile,
    *scratch,
):
    run, wins, groups, own, listed, dims = cfg
    bufs = scratch[:run]
    rowbs = scratch[run : 2 * run]
    red, send_sem, recv_sem, red_send, red_recv = scratch[2 * run :]
    dim_z, dim_y, dim_x = dims
    devices = wins * groups
    windows = wins * run
    win = lax.axis_index("win")
    grp = lax.axis_index("grp")
    me = win * groups + grp
    my_z = grp // (dim_y * dim_x)
    my_y = (grp // dim_x) % dim_y
    my_x = grp % dim_x
    two_ends = wins == 2 and run == 2

    def window_of(slot):
        if two_ends:
            return jnp.where(win == 0, 1 - slot, slot)
        return slot

    def at(dz, dy, dx):
        return (
            ((my_z + dz) % dim_z) * dim_y + (my_y + dy) % dim_y
        ) * dim_x + (my_x + dx) % dim_x

    barrier = pltpu.get_barrier_semaphore()

    def greet(step, carry):
        other = (me + step) % devices
        pl.semaphore_signal(
            barrier, inc=1, device_id=(other // groups, other % groups), device_id_type=MESH
        )
        return carry

    lax.fori_loop(1, devices, greet, 0)

    def spread(slot):
        local = window_of(slot)

        def one(block, carry):
            start = pl.multiple_of(block * TILE, TILE)
            tile = table[local, :, pl.ds(start, TILE)]
            packed = jnp.concatenate(
                [tile[0:4], 4.0 * tile[4:5], 1.0 / tile[5:6], tile[0:2]], axis=0
            )
            turned = jnp.transpose(packed)
            for field in range(FIELDS):
                wide = jnp.broadcast_to(turned[:, field : field + 1], (TILE, TILE))
                for piece in range(PIECES):
                    rowbs[slot][(block * FIELDS + field) * PIECES + piece] = wide[
                        piece * ROWS : (piece + 1) * ROWS
                    ]
            return carry

        lax.fori_loop(0, own, one, 0)

    def pack(block, carry):
        start = pl.multiple_of(block * TILE, TILE)
        for slot in range(run):
            tile = table[window_of(slot), :, pl.ds(start, TILE)]
            for field in range(FIELDS):
                bufs[slot][(grp * own + block) * FIELDS + field] = tile[field : field + 1]
        return carry

    lax.fori_loop(0, own, pack, 0)

    shares = []
    lowers = []
    for wl in range(run):
        window = win * run + wl
        odd = (window + parity[0]) & 1
        lower = window - odd
        threshold = thresholds[0]
        for v in range(1, windows):
            threshold = jnp.where(lower == v, thresholds[v], threshold)
        drawn = ((threshold + parity[0]) & 1073741823) + 1
        share = jnp.full((ROWS, TILE), drawn, jnp.int32).astype(jnp.float32) * (1.0 / 1073741824.0)
        shares.append(-jnp.log(share))
        lowers.append(lower)

    pl.semaphore_wait(barrier, devices - 1)

    counts = [0] * run

    def share_of(slot, owner):
        return bufs[slot].at[pl.ds(owner * (own * FIELDS), own * FIELDS)]

    def descriptor(slot, owner, target, number):
        return pltpu.make_async_remote_copy(
            src_ref=share_of(slot, owner),
            dst_ref=share_of(slot, owner),
            send_sem=send_sem.at[slot, number],
            recv_sem=recv_sem.at[slot, owner],
            device_id={"grp": target},
            device_id_type=MESH,
        )

    sent = []

    def send(slot, owner, target):
        copy = descriptor(slot, owner, target, counts[slot])
        counts[slot] += 1
        copy.start()
        sent.append(copy)

    def arrived(slot, owner):
        descriptor(slot, owner, owner, 0).wait_recv()

    def to_x(slot, owner):
        for dx in range(1, dim_x):
            send(slot, owner, at(0, 0, dx))

    def to_y(slot, owner):
        for dy in range(1, dim_y):
            send(slot, owner, at(0, dy, 0))

    def open_sends(slot):
        for dz in range(1, dim_z):
            send(slot, grp, at(dz, 0, 0))
        to_x(slot, grp)
        to_y(slot, grp)

    def pass_plane(slot, dz):
        for dx in range(1, dim_x):
            owner = at(dz, 0, dx)
            arrived(slot, owner)
            if dz % 2 == 0:
                to_y(slot, owner)
        for dy in range(1, dim_y):
            owner = at(dz, dy, 0)
            arrived(slot, owner)
            if dz % 2 == 1:
                to_x(slot, owner)

    def pass_column(slot):
        for dz in range(1, dim_z):
            owner = at(dz, 0, 0)
            arrived(slot, owner)
            to_x(slot, owner)
            to_y(slot, owner)

    def pass_planes(slot):
        for dz in range(dim_z):
            pass_plane(slot, dz)

    def last_arrivals(slot):
        for dz in range(dim_z):
            for dy in range(1, dim_y):
                for dx in range(1, dim_x):
                    arrived(slot, at(dz, dy, dx))

    def lambda_list(slot):
        window = win * run + window_of(slot)
        if two_ends and slot == 1:
            low = jnp.where(window == 0, 0, window - 1)
            return [lambdas[low], lambdas[low + 1]]
        return [
            lambdas[jnp.maximum(window - 1, 0)],
            lambdas[window],
            lambdas[jnp.minimum(window + 1, windows - 1)],
        ]

    def start_state(slot):
        zero = jnp.zeros((ROWS, TILE), jnp.float32)
        row = jnp.zeros((1, TILE), jnp.float32)
        return tuple(zero for _ in lambda_list(slot)) + (row, row)

    def tiles(slot, first, last, state):
        local = window_of(slot)
        lams = lambda_list(slot)
        cores = [1.0 - 0.5 * lam for lam in lams]
        softs = [2.0 - lam for lam in lams]
        base = grp * own

        def one(pair, state):
            row_id = row_ids[local, pair]
            col_id = col_ids[local, pair]
            first_row = col_id * FIELDS
            col = [bufs[slot][first_row + f] for f in range(FIELDS)]
            mine = jnp.clip(row_id - base, 0, own - 1) * (FIELDS * PIECES)
            fields = [jnp.broadcast_to(col[f], (ROWS, TILE)) for f in range(3)]
            charge_col = col[3]
            depth_col = col[4]
            size_col = jnp.broadcast_to(1.0 / col[5], (ROWS, TILE))
            sum_disp = [None] * len(lams)
            sum_coul = [None] * len(lams)
            for piece in range(TILE // ROWS):
                dx = rowbs[slot][mine + piece] - fields[0]
                dy = rowbs[slot][mine + 1 * PIECES + piece] - fields[1]
                dz = rowbs[slot][mine + 2 * PIECES + piece] - fields[2]
                charge = rowbs[slot][mine + 3 * PIECES + piece]
                depth = rowbs[slot][mine + 4 * PIECES + piece]
                r2 = dx * dx + dy * dy + dz * dz
                scaled = r2 * (rowbs[slot][mine + 5 * PIECES + piece] * size_col)
                cube = scaled * scaled * scaled
                for k in range(len(lams)):
                    root = lax.rsqrt(cube + cores[k])
                    inverse = root * root
                    disp = (depth * inverse) * (inverse - 1.0)
                    coul = charge * lax.rsqrt(r2 + softs[k])
                    if piece == 0:
                        sum_disp[k], sum_coul[k] = disp, coul
                    else:
                        sum_disp[k] = sum_disp[k] + disp
                        sum_coul[k] = sum_coul[k] + coul
            totals = [
                state[k] + (sum_disp[k] * depth_col + sum_coul[k] * charge_col)
                for k in range(len(lams))
            ]
            same = jnp.where(row_id == col_id, 1.0, 0.0)
            return tuple(totals) + (
                state[-2] + same * (depth_col * depth_col),
                state[-1] + same * (charge_col * charge_col),
            )

        return lax.fori_loop(first, last, one, state)

    def close(slot, state):
        out = []
        for k, lam in enumerate(lambda_list(slot)):
            core = jnp.full((1, TILE), 1.0 - 0.5 * lam, jnp.float32)
            soft = jnp.full((1, TILE), 2.0 - lam, jnp.float32)
            inverse = 1.0 / core
            own_pairs = state[-2] * (4.0 * inverse * (inverse - 1.0)) + state[-1] * lax.rsqrt(soft)
            line = jnp.sum(state[k], axis=0, keepdims=True) - own_pairs
            out.append(jnp.sum(line, axis=1, keepdims=True) * lam)
        if two_ends and slot == 1:
            out = [out[0], jnp.where(win == 0, out[0], out[1]), out[1]]
        return out

    open_sends(0)
    spread(0)
    pass_column(0)
    for slot in range(1, run):
        open_sends(slot)
    pass_planes(0)
    if run > 1:
        pass_column(1)
    for slot in range(1, run):
        spread(slot)
    last_arrivals(0)
    partial = []
    for slot in range(run):
        state = start_state(slot)
        if slot + 1 < run:
            half = (3 * listed) // 8
            state = tiles(slot, 0, half, state)
            if slot > 0:
                pass_column(slot + 1)
            pass_planes(slot + 1)
            state = tiles(slot, half, listed, state)
            last_arrivals(slot + 1)
        else:
            state = tiles(slot, 0, listed, state)
        partial.append(close(slot, state))

    lane = lax.broadcasted_iota(jnp.int32, (1, TILE), 1)
    line = jnp.zeros((1, TILE), jnp.float32)
    for slot in range(run):
        place = window_of(slot) * 3
        for k in range(3):
            line = jnp.where(lane == place + k, partial[slot][k], line)
    red[me] = line

    def share_out(step, carry):
        other = (me + step) % devices
        pltpu.make_async_remote_copy(
            src_ref=red.at[me],
            dst_ref=red.at[me],
            send_sem=red_send.at[step],
            recv_sem=red_recv.at[me],
            device_id=(other // groups, other % groups),
            device_id_type=MESH,
        ).start()
        return carry

    lax.fori_loop(1, devices, share_out, 0)
    for copy in sent:
        copy.wait_send()

    def collect(step, carry):
        other = (me + step) % devices
        copy = pltpu.make_async_remote_copy(
            src_ref=red.at[other],
            dst_ref=red.at[other],
            send_sem=red_send.at[step],
            recv_sem=red_recv.at[other],
            device_id=(other // groups, other % groups),
            device_id_type=MESH,
        )
        copy.wait_recv()
        copy.wait_send()
        return carry

    lax.fori_loop(1, devices, collect, 0)
    scale = 1.0 / (listed * groups * TILE * TILE)
    energy = []
    for part in range(wins):
        total = jnp.sum(red[part * groups : (part + 1) * groups], axis=0) * scale
        for wl in range(run):
            energy.append(
                [jnp.sum(jnp.where(lane == wl * 3 + k, total, 0.0)) for k in range(3)]
            )
    ups = [e[2] - e[1] for e in energy]
    downs = [e[0] - e[1] for e in energy]
    for wl in range(run):
        window = win * run + wl
        for k in range(3):
            value = energy[wl][k]
            for part in range(1, wins):
                value = jnp.where(win == part, energy[part * run + wl][k], value)
            out_energy[wl, k] = value
        profile = jnp.float32(0.0)
        change = jnp.float32(0.0)
        for v in range(windows):
            profile = profile + jnp.where(v < window, ups[v], 0.0)
            change = change + jnp.where(lowers[wl] == v, ups[v], 0.0)
            change = change + jnp.where(lowers[wl] + 1 == v, downs[v], 0.0)
        out_profile[wl] = profile
        partner = jnp.logical_and(lowers[wl] >= 0, lowers[wl] + 1 < windows)
        margin = jnp.max(shares[wl]) - inverse_temp[0] * change
        out_margin[wl] = jnp.where(partner, margin, 0.0)


def per_device(dims, atom_table, row_blocks, col_blocks, lambdas, inverse_temp, parity, thresholds):
    run, fields, atoms = atom_table.shape
    wins = lax.axis_size("win")
    groups = lax.axis_size("grp")
    own = atoms // TILE
    listed = row_blocks.shape[1]
    cfg = (run, wins, groups, own, listed, dims)
    smem = pl.BlockSpec(memory_space=pltpu.SMEM)
    vmem = pl.BlockSpec(memory_space=pltpu.VMEM)
    devices = wins * groups
    scratch = [pltpu.VMEM((groups * own * fields, 1, TILE), jnp.float32) for _ in range(run)]
    scratch += [pltpu.VMEM((own * FIELDS * PIECES, ROWS, TILE), jnp.float32) for _ in range(run)]
    scratch += [
        pltpu.VMEM((devices, 1, TILE), jnp.float32),
        pltpu.SemaphoreType.DMA((run, max(1, messages_of(dims)))),
        pltpu.SemaphoreType.DMA((run, groups)),
        pltpu.SemaphoreType.DMA((devices,)),
        pltpu.SemaphoreType.DMA((devices,)),
    ]
    return pl.pallas_call(
        functools.partial(kernel, cfg),
        out_shape=(
            jax.ShapeDtypeStruct((run, 3), jnp.float32),
            jax.ShapeDtypeStruct((run,), jnp.float32),
            jax.ShapeDtypeStruct((run,), jnp.float32),
        ),
        in_specs=[vmem, smem, smem, smem, smem, smem, smem],
        out_specs=(smem, smem, smem),
        scratch_shapes=scratch,
        compiler_params=pltpu.CompilerParams(
            collective_id=0, has_side_effects=True, vmem_limit_bytes=48 * 1024 * 1024
        ),
    )(atom_table, row_blocks, col_blocks, lambdas, inverse_temp, parity, thresholds)


def solution(mesh):
    return jax.shard_map(
        functools.partial(per_device, grid_of(mesh)),
        mesh=mesh,
        in_specs=(P("win", None, "grp"), P("win", "grp"), P("win", "grp"), P(), P(), P(), P()),
        out_specs=(P("win", None), P("win"), P("win")),
        check_vma=False,
    )
```
